128 devices in a mesh: gx: 32 (over x, y, core), gy: 4 (over z).
Axes of the slice: x: 4, y: 4, z: 4, core: 2. Of those that a mesh axis runs over, the one named last changes fastest.
Arguments:
- candidate_owner: int32 [1024, 512, 1], P(('gx', 'gy')), may hold values from 0 to 127; in each aligned block of 4096 rows (0 to 4095, 4096 to 8191, ..., all dimensions but the last counted through in order) at most 64 rows name the same one
- candidate_row: int32 [1024, 512], P(('gx', 'gy')), may hold values from 0 to 78335
- item_table: bfloat16 [10027008, 128], P(('gx', 'gy')), may hold values from -6 to 6
- w_in: bfloat16 [128, 512], replicated, may hold values from -0.5 to 0.5
- w_qkv: bfloat16 [1, 512, 1536], replicated, may hold values from -0.25 to 0.25
- w_out: bfloat16 [1, 512, 512], replicated, may hold values from -0.25 to 0.25
- w_up: bfloat16 [1, 512, 1024], replicated, may hold values from -0.25 to 0.25
- w_down: bfloat16 [1, 1024, 512], replicated, may hold values from -0.1875 to 0.1875
- norm_gains: float32 [1, 2, 512], replicated, may hold values from 0.25 to 1.75
- final_gain: float32 [512], replicated, may hold values from 0.25 to 1.75
- w_score: bfloat16 [512], replicated, may hold values from -0.25 to 0.25
Outputs:
- log_probs: float32 [1024, 512], P(('gx', 'gy'))
The draws below stay inside these ranges and needn't reach their ends.
Inputs may be any that keep to these rules, and one draw needn't show every extreme that they name: `candidate_owner`: among the candidates of one device's 8 slates no shard is named more than 64 times, a bound that some block reaches.
All inputs are finite; a program needn't handle non-finite values.
Results may differ from the reference program's by a relative error of at most 0.0007.
Values may be sent and summed in bfloat16 or wider, within the bound.
A program may use at most 128 MiB of HBM per device.

```python
import math
import jax
import jax.numpy as jnp
import numpy as np
from jax import lax

SLATE_LEN = 512
SLATES_DEV = 8
SLATES = 1024
EMB = 128
ROWS_DEV = 78336
ROWS = 10027008
D = 512
HEADS = 8
FF = 1024
LAYERS = 1
CAP = 64
N_GX = 32
N_GY = 4


def set_ends(values, rng, smallest, largest):
    dims = values.shape
    place = [jax.random.randint(jax.random.fold_in(rng, axis), (), 0, dims[axis]) for axis in range(len(dims))]
    values = values.at[tuple(place)].set(smallest)
    longest = dims.index(max(dims))
    place[longest] = (place[longest] + 1) % dims[longest]
    return values.at[tuple(place)].set(largest)


def shard_levels(stream_key, shape, split, smallest, high):
    level, own = 1.0, jax.random.fold_in(stream_key, 6)
    for position, shards_of in split:
        steps = jnp.exp(jax.random.uniform(jax.random.fold_in(own, position), (shards_of,), jnp.float32, smallest / len(split), high / len(split)))
        level = level * jnp.repeat(steps, shape[position] // shards_of).reshape([-1 if axis == position else 1 for axis in range(len(shape))])
    return level


def wide_ids(key, dims, number_of, slope):
    portions = [min(1 << octave, number_of + 1 - (1 << octave)) * (1 << 20) // math.isqrt((1 << octave) ** slope) + 1 for octave in range((number_of + 1).bit_length()) if 1 << octave <= number_of]
    spread = 1 + sum(portions) // (1 << 30)
    listing = np.cumsum(np.array([max(1, weight // spread) for weight in portions]))
    pick = jax.random.randint(jax.random.fold_in(key, 1), dims, 0, int(listing[len(portions) - 1]))
    start = jnp.left_shift(1, jnp.searchsorted(jnp.asarray(listing, jnp.int32), pick, side="right").astype(jnp.int32))
    grade = start - 1 + jax.random.randint(jax.random.fold_in(key, 4), dims, 0, 1 << 30) % jnp.minimum(start, number_of + 1 - start)
    return jax.random.permutation(jax.random.fold_in(key, 2), number_of)[grade].astype(jnp.int32)


def deal_out(rng, own, number, rows, number_of, top, bound, skew):
    sequence = jax.random.permutation(rng, number_of)
    packed, common = load_shares(number_of, rows * top, bound, skew, True), load_shares(number_of, rows * top, bound, skew, False)
    places = jnp.arange(number_of)

    def named(lengths, turn):
        used = int((lengths > 0).sum())
        fixed = max(1, used // 4)
        moved = fixed + (places - fixed + turn * (used - fixed)) % max(1, number_of - fixed)
        return jnp.zeros((number_of,), jnp.int32).at[sequence[jnp.where(places < fixed, places, moved)]].set(jnp.asarray(lengths, jnp.int32))

    lengths = jnp.where(number % 4 == 0, named(packed, number // 4), named(common, number - number // 4 - 1))
    mixed = jax.random.permutation(jax.random.fold_in(own, 3), number_of)
    source_of, sink = mixed[0:number_of // 2 * 2:2], mixed[1:number_of // 2 * 2:2]
    room = jnp.minimum(lengths[source_of] - 1, bound - lengths[sink]) // 2
    room = jnp.where((source_of == sequence[0]) | (sink == sequence[0]) | (lengths[sink] == 0), 0, jnp.maximum(room, 0))
    moved = jax.random.randint(jax.random.fold_in(own, 4), (number_of // 2,), 0, 1 << 20) % (room + 1)
    lengths = lengths.at[source_of].add(-moved).at[sink].add(moved)
    members = jnp.searchsorted(jnp.cumsum(lengths), jnp.arange(rows * top), side="right").astype(jnp.int32)
    grid = members.reshape(top, rows).T
    grid = grid[jax.random.permutation(jax.random.fold_in(own, 1), rows)]
    turn = jax.random.randint(jax.random.fold_in(own, 2), (rows, 1), 0, top)
    return jnp.take_along_axis(grid, (jnp.arange(top)[None, :] + turn) % top, axis=1)


def load_shares(amount, total, limit, lean, full):
    portions = [(1 << 20) // math.isqrt(standing ** lean) + 1 for standing in range(1, amount + 1)]
    largest = limit if full else min(limit, max(-(-total // amount), total * portions[0] // sum(portions)))
    least = 1 if total - largest >= amount - 1 else 0
    holding, rest = [largest] + [least] * (amount - 1), total - largest - least * (amount - 1)
    while rest > 0:
        free = [i for i in range(1, amount) if holding[i] < largest] or [i for i in range(1, amount) if holding[i] < limit]
        pool, budget = sum([portions[i] for i in free]), rest
        for i in free:
            addition = min(limit - holding[i], max(1, budget * portions[i] // pool), rest)
            holding[i] = holding[i] + addition
            rest = rest - addition
    return np.array(holding)


def normal_values(own_key, extent, scale, most, pieces=(), dtype=jnp.bfloat16):
    factor_of = shard_levels(own_key, extent, pieces, -0.22, 0.18) if pieces else 1.0
    drawn = jax.random.normal(own_key, extent, jnp.float32) * scale * factor_of
    return jnp.minimum(jnp.maximum(drawn, -most), most).astype(dtype)


def setup_inputs(seed: int = 0) -> dict:
    arg_keys = jax.random.split(jax.random.key(seed), 12)
    candidate_owner_keys = jax.random.split(jax.random.fold_in(arg_keys[0], 1), SLATES * SLATE_LEN // (SLATES_DEV * SLATE_LEN))
    candidate_owner_turns = jax.random.permutation(jax.random.fold_in(arg_keys[0], 3), SLATES * SLATE_LEN // (SLATES_DEV * SLATE_LEN))
    candidate_owner = jax.vmap(lambda own, number: deal_out(jax.random.fold_in(arg_keys[0], 2), own, number, SLATES_DEV * SLATE_LEN, N_GX * N_GY, 1, CAP, 2))(candidate_owner_keys, candidate_owner_turns).reshape((SLATES, SLATE_LEN, 1))
    candidate_row = set_ends(wide_ids(arg_keys[1], (SLATES, SLATE_LEN), ROWS_DEV, 2), jax.random.fold_in(arg_keys[1], 3), 0, ROWS_DEV - 1).astype(jnp.int32)
    item_table = normal_values(arg_keys[2], (ROWS, EMB), 1.0, 6.0, ((0, 128),))
    w_in = normal_values(arg_keys[3], (EMB, D), EMB ** -0.5, 0.5)
    w_qkv = normal_values(arg_keys[4], (LAYERS, D, 3 * D), D ** -0.5, 0.25)
    w_out = normal_values(arg_keys[5], (LAYERS, D, D), D ** -0.5, 0.25)
    w_up = normal_values(arg_keys[6], (LAYERS, D, FF), D ** -0.5, 0.25)
    w_down = normal_values(arg_keys[7], (LAYERS, FF, D), FF ** -0.5, 0.1875)
    norm_gains = jnp.clip(1.0 + 0.15 * jax.random.normal(arg_keys[8], (LAYERS, 2, D), jnp.float32), 0.25, 1.75)
    final_gain = jnp.clip(1.0 + 0.15 * jax.random.normal(arg_keys[9], (D,), jnp.float32), 0.25, 1.75)
    w_score = normal_values(arg_keys[10], (D,), D ** -0.5, 0.25)
    return dict(candidate_owner=candidate_owner, candidate_row=candidate_row, item_table=item_table, w_in=w_in, w_qkv=w_qkv, w_out=w_out, w_up=w_up, w_down=w_down, norm_gains=norm_gains, final_gain=final_gain, w_score=w_score)


def layer_norm(values, gain):
    mean = lax.optimization_barrier(jnp.mean(values, axis=-1, keepdims=True))
    centred = values - mean
    variance = lax.optimization_barrier(jnp.mean(centred * centred, axis=-1, keepdims=True))
    return centred * lax.rsqrt(variance + 1e-05) * gain

def score_slates(emb, w_in, w_qkv, w_out, w_up, w_down, norm_gains, final_gain, w_score):
    slates, length, width = emb.shape
    model = w_in.shape[1]
    head_dim = model // HEADS
    resid = jnp.dot(emb.reshape(slates * length, width), w_in, preferred_element_type=jnp.float32)
    for layer in range(LAYERS):
        normed = layer_norm(resid, norm_gains[layer, 0]).astype(jnp.bfloat16)
        qkv = jnp.dot(normed, w_qkv[layer], preferred_element_type=jnp.float32).astype(jnp.bfloat16)
        qkv = qkv.reshape(slates, length, 3, HEADS, head_dim)
        query = qkv[:, :, 0].astype(jnp.float32)
        keys = qkv[:, :, 1].astype(jnp.float32)
        values = qkv[:, :, 2].astype(jnp.float32)
        scores = jnp.einsum('bqhd,bkhd->bhqk', query, keys) * head_dim ** (-0.5)
        probs = jax.nn.softmax(scores, axis=-1).astype(jnp.bfloat16)
        mixed = jnp.einsum('bhqk,bkhd->bqhd', probs.astype(jnp.float32), values)
        mixed = mixed.astype(jnp.bfloat16).reshape(slates * length, model)
        resid = resid + jnp.dot(mixed, w_out[layer], preferred_element_type=jnp.float32)
        normed = layer_norm(resid, norm_gains[layer, 1]).astype(jnp.bfloat16)
        inner = jax.nn.gelu(jnp.dot(normed, w_up[layer], preferred_element_type=jnp.float32)).astype(jnp.bfloat16)
        resid = resid + jnp.dot(inner, w_down[layer], preferred_element_type=jnp.float32)
    final = layer_norm(resid, final_gain)
    logits = lax.optimization_barrier(jnp.sum(final * w_score.astype(jnp.float32)[None, :], axis=-1))
    return jax.nn.log_softmax(logits.reshape(slates, length), axis=-1)

def reference(candidate_owner, candidate_row, item_table, w_in, w_qkv, w_out, w_up, w_down, norm_gains, final_gain, w_score):
    item = (candidate_owner[:, :, 0] * ROWS_DEV + candidate_row).astype(jnp.int32)
    emb = jnp.take(item_table, item.reshape(-1), axis=0)
    emb = emb.reshape(N_GX * N_GY * SLATES_DEV, 1, SLATE_LEN, EMB)

    def one_group(block):
        return score_slates(block, w_in, w_qkv, w_out, w_up, w_down, norm_gains, final_gain, w_score)
    scored = lax.map(one_group, emb)
    return scored.reshape(SLATES, SLATE_LEN)
```

```python
import functools

import jax
import jax.numpy as jnp
from jax import lax
from jax.experimental import pallas as pl
from jax.experimental.pallas import tpu as pltpu
from jax.sharding import PartitionSpec as P

HEADS = 8
MESH = pl.DeviceIdType.MESH


def layer_norm(values, gain):
    mean = jnp.mean(values, axis=-1, keepdims=True)
    centred = values - mean
    variance = jnp.mean(centred * centred, axis=-1, keepdims=True)
    return centred * lax.rsqrt(variance + 1e-05) * gain


def slate_kernel(
    emb_ref, w_in_ref, w_qkv_ref, w_out_ref, w_up_ref, w_down_ref, gains_ref, final_ref, score_ref,
    out_ref, qkv_ref, mixed_ref,
):
    length, model = mixed_ref.shape
    resid = jnp.dot(emb_ref[...], w_in_ref[...], preferred_element_type=jnp.float32)
    normed = layer_norm(resid, gains_ref[0:1, :]).astype(jnp.bfloat16)
    qkv_ref[...] = jnp.dot(normed, w_qkv_ref[...], preferred_element_type=jnp.float32).astype(
        jnp.bfloat16
    )
    low = lax.broadcasted_iota(jnp.int32, (1, 128), 1) < 64
    scales = (
        jnp.where(low, 0.125, 0.0).astype(jnp.bfloat16),
        jnp.where(low, 0.0, 0.125).astype(jnp.bfloat16),
    )
    ones = jnp.ones((length, 128), jnp.bfloat16)
    for first in range(0, model, 128):
        query = qkv_ref[:, first : first + 128]
        keys = qkv_ref[:, model + first : model + first + 128]
        values = qkv_ref[:, 2 * model + first : 2 * model + first + 128]
        values = jnp.concatenate([values, ones], axis=1)
        heads = []
        for scale in scales:
            scores = lax.dot_general(
                query * scale, keys, (((1,), (1,)), ((), ())), preferred_element_type=jnp.float32
            )
            top = jnp.max(scores, axis=-1, keepdims=True)
            weights = jnp.exp(scores - top).astype(jnp.bfloat16)
            both = jnp.dot(weights, values, preferred_element_type=jnp.float32)
            heads.append(both[:, :128] / both[:, 128:])
        mixed_ref[:, first : first + 128] = jnp.where(low, heads[0], heads[1]).astype(jnp.bfloat16)
    resid = resid + jnp.dot(mixed_ref[...], w_out_ref[...], preferred_element_type=jnp.float32)
    normed = layer_norm(resid, gains_ref[1:2, :]).astype(jnp.bfloat16)
    inner = jax.nn.gelu(
        jnp.dot(normed, w_up_ref[...], preferred_element_type=jnp.float32)
    ).astype(jnp.bfloat16)
    resid = resid + jnp.dot(inner, w_down_ref[...], preferred_element_type=jnp.float32)
    final = layer_norm(resid, final_ref[...])
    logits = jnp.sum(final * score_ref[...].astype(jnp.float32), axis=-1).reshape(1, length)
    shifted = logits - jnp.max(logits, axis=-1, keepdims=True)
    total = jnp.sum(jnp.exp(shifted), axis=-1, keepdims=True)
    out_ref[...] = (shifted - jnp.log(total))[None]


def score_slates(emb, w_in, w_qkv, w_out, w_up, w_down, norm_gains, final_gain, w_score):
    slates, length, width = emb.shape
    model = w_in.shape[1]
    whole = (
        w_in, w_qkv[0], w_out[0], w_up[0], w_down[0], norm_gains[0], final_gain[None], w_score[None],
    )
    scored = pl.pallas_call(
        slate_kernel,
        grid=(slates,),
        in_specs=[pl.BlockSpec((length, width), lambda i: (i, 0))]
        + [pl.BlockSpec(a.shape, lambda i: (0, 0)) for a in whole],
        out_specs=pl.BlockSpec((1, 1, length), lambda i: (i, 0, 0)),
        out_shape=jax.ShapeDtypeStruct((slates, 1, length), jnp.float32),
        scratch_shapes=[
            pltpu.VMEM((length, 3 * model), jnp.bfloat16),
            pltpu.VMEM((length, model), jnp.bfloat16),
        ],
        compiler_params=pltpu.CompilerParams(vmem_limit_bytes=40 * 1024 * 1024),
        name="slates",
    )(emb.reshape(slates * length, width), *whole)
    return scored.reshape(slates, length)


def slot_numbers(owner, shards, length):
    total = owner.shape[0]
    onehot = (owner[:, None] == jnp.arange(shards, dtype=jnp.int32)[None, :]).astype(jnp.bfloat16)
    blocks = onehot.reshape(total // length, length, shards)
    lower = (jnp.arange(length)[:, None] >= jnp.arange(length)[None, :]).astype(jnp.bfloat16)
    within = jnp.einsum("ij,bjn->bin", lower, blocks, preferred_element_type=jnp.float32)
    totals = within[:, -1, :]
    before = jnp.cumsum(totals, axis=0) - totals
    counts = within + before[:, None, :]
    picked = jnp.sum(counts * blocks.astype(jnp.float32), axis=-1)
    return (picked.reshape(total) - 1.0).astype(jnp.int32)


def peer(step):
    gx, gy = lax.axis_index("gx"), lax.axis_index("gy")
    x, y, core = gx // 8, (gx // 2) % 4, gx % 2
    to_x, to_y = (x + step % 4) % 4, (y + (step // 4) % 4) % 4
    to_z, to_core = (gy + (step // 16) % 4) % 4, (core + step // 64) % 2
    to_gx = (to_x * 4 + to_y) * 2 + to_core
    return to_gx, to_z, to_gx * 4 + to_z


def exchange_kernel(
    want_ref, table_ref, out_ref, packed, table, block, sending, asked, numbers,
    chunk_sems, ask_send, ask_recv, row_send, row_recv, number_sem, *, shards, chunks, capacity,
):
    length = table_ref.shape[0] // chunks
    me = lax.axis_index("gx") * 4 + lax.axis_index("gy")

    def chunk_copy(chunk):
        piece = pl.ds(chunk * length, length)
        return pltpu.make_async_copy(table_ref.at[piece], packed.at[piece], chunk_sems.at[chunk])

    for chunk in range(chunks):
        chunk_copy(chunk).start()
    barrier = pltpu.get_barrier_semaphore()

    def greet(step, carry):
        to_gx, to_gy, _ = peer(step)
        pl.semaphore_signal(barrier, inc=1, device_id=(to_gx, to_gy), device_id_type=MESH)
        return carry

    lax.fori_loop(1, shards, greet, 0)
    pl.semaphore_wait(barrier, shards - 1)

    def ask(step, carry):
        to_gx, to_gy, shard = peer(step)
        pltpu.make_async_remote_copy(
            src_ref=want_ref.at[shard], dst_ref=asked.at[me], send_sem=ask_send, recv_sem=ask_recv,
            device_id=(to_gx, to_gy), device_id_type=MESH,
        ).start()
        return carry

    lax.fori_loop(1, shards, ask, 0)
    asked[pl.ds(me, 1)] = want_ref[pl.ds(me, 1)]
    for chunk in range(chunks):
        chunk_copy(chunk).wait()

        def widen(part, carry):
            piece = pl.ds(chunk * length + part * 128, 128)
            table[piece] = packed[piece].astype(jnp.float32)
            return carry

        lax.fori_loop(0, length // 128, widen, 0)
    others = pl.ds(0, shards - 1)
    pltpu.make_async_copy(asked.at[others], asked.at[others], ask_recv).wait()
    pltpu.make_async_copy(asked.at[others], asked.at[others], ask_send).wait()
    copy = pltpu.make_async_copy(asked, numbers, number_sem)
    copy.start()
    copy.wait()

    def collect(shard, target):
        for slot in range(capacity):
            block[pl.ds(slot, 1)] = table[pl.ds(numbers[shard, 0, slot], 1)]
        target[...] = block[...].astype(jnp.bfloat16)

    def give(step, carry):
        to_gx, to_gy, shard = peer(step)
        collect(shard, sending.at[shard])
        pltpu.make_async_remote_copy(
            src_ref=sending.at[shard], dst_ref=out_ref.at[me], send_sem=row_send, recv_sem=row_recv,
            device_id=(to_gx, to_gy), device_id_type=MESH,
        ).start()
        return carry

    lax.fori_loop(1, shards, give, 0)
    collect(me, out_ref.at[me])
    pltpu.make_async_copy(out_ref.at[others], out_ref.at[others], row_recv).wait()
    pltpu.make_async_copy(out_ref.at[others], out_ref.at[others], row_send).wait()


def exchange(want, item_table, capacity):
    shards, _, lanes = want.shape
    rows, width = item_table.shape
    chunks = 6
    return pl.pallas_call(
        functools.partial(exchange_kernel, shards=shards, chunks=chunks, capacity=capacity),
        in_specs=[pl.BlockSpec(memory_space=pltpu.VMEM), pl.BlockSpec(memory_space=pl.ANY)],
        out_specs=pl.BlockSpec(memory_space=pltpu.VMEM),
        out_shape=jax.ShapeDtypeStruct((shards, capacity, width), jnp.bfloat16),
        scratch_shapes=[
            pltpu.VMEM((rows, width), jnp.bfloat16),
            pltpu.VMEM((rows, width), jnp.float32),
            pltpu.VMEM((capacity, width), jnp.float32),
            pltpu.VMEM((shards, capacity, width), jnp.bfloat16),
            pltpu.VMEM((shards, 1, lanes), jnp.int32),
            pltpu.SMEM((shards, 1, lanes), jnp.int32),
            pltpu.SemaphoreType.DMA((chunks,)),
            pltpu.SemaphoreType.DMA,
            pltpu.SemaphoreType.DMA,
            pltpu.SemaphoreType.DMA,
            pltpu.SemaphoreType.DMA,
            pltpu.SemaphoreType.DMA,
        ],
        compiler_params=pltpu.CompilerParams(
            collective_id=0, has_side_effects=True, vmem_limit_bytes=67043328
        ),
        name="exchange",
    )(want, item_table)


def per_device(
    candidate_owner,
    candidate_row,
    item_table,
    w_in,
    w_qkv,
    w_out,
    w_up,
    w_down,
    norm_gains,
    final_gain,
    w_score,
):
    slates, length, unused = candidate_owner.shape
    width = item_table.shape[1]
    shards = lax.axis_size(("gx", "gy"))
    capacity = max(2, 2 * slates * length // shards)
    owner = candidate_owner.reshape(slates * length)
    row_index = candidate_row.reshape(slates * length)
    slot = slot_numbers(owner, shards, length)
    lanes = 128
    wanted = jnp.zeros((shards * lanes,), jnp.int32).at[owner * lanes + slot].set(row_index)
    returned = exchange(wanted.reshape(shards, 1, lanes), item_table, capacity)
    returned = returned.reshape(shards * capacity, width)
    position = owner * capacity + slot
    emb = jnp.take(returned, position, axis=0).reshape(slates, length, width)
    return score_slates(emb, w_in, w_qkv, w_out, w_up, w_down, norm_gains, final_gain, w_score)


def solution(mesh):
    return jax.shard_map(
        per_device,
        mesh=mesh,
        in_specs=(
            P(("gx", "gy"), None, None),
            P(("gx", "gy"), None),
            P(("gx", "gy"), None),
            P(),
            P(),
            P(),
            P(),
            P(),
            P(),
            P(),
            P(),
        ),
        out_specs=P(("gx", "gy"), None),
        check_vma=False,
    )
```

```python
import functools

import jax
import jax.numpy as jnp
from jax import lax
from jax.experimental import pallas as pl
from jax.experimental.pallas import tpu as pltpu
from jax.sharding import PartitionSpec as P

MESH = pl.DeviceIdType.MESH


def layer_norm(values, gain):
    mean = jnp.mean(values, axis=-1, keepdims=True)
    centred = values - mean
    variance = jnp.mean(centred * centred, axis=-1, keepdims=True)
    return centred * lax.rsqrt(variance + 1e-05) * gain


def slate_kernel(
    place_ref, rows_ref, w_in_ref, w_qkv_ref, w_out_ref, w_up_ref, w_down_ref, gains_ref, final_ref,
    score_ref, out_ref, qkv_ref, mixed_ref, wide_ref, emb_ref, *, block,
):
    length, model = mixed_ref.shape
    step = pl.program_id(0)
    now, later = step % 2, (step + 1) % 2
    following = jnp.minimum(step + 1, pl.num_programs(0) - 1)

    @pl.when(step == 0)
    def _():
        def widen(part, carry):
            piece = pl.ds(pl.multiple_of(part * 128, 128), 128)
            wide_ref[piece] = rows_ref[piece].astype(jnp.float32)
            return carry

        lax.fori_loop(0, rows_ref.shape[0] // 128, widen, 0)

        def fetch(part, carry):
            first = pl.multiple_of(part * 32, 32)
            for r in range(32):
                emb_ref[0, pl.ds(first + r, 1)] = wide_ref[pl.ds(place_ref[0, 0, first + r], 1)]
            return carry

        lax.fori_loop(0, length // 32, fetch, 0)

    emb = emb_ref[now].astype(jnp.bfloat16)
    resid = jnp.dot(emb, w_in_ref[...], preferred_element_type=jnp.float32)
    normed = layer_norm(resid, gains_ref[0:1, :]).astype(jnp.bfloat16)
    qkv_ref[...] = jnp.dot(normed, w_qkv_ref[...], preferred_element_type=jnp.float32).astype(
        jnp.bfloat16
    )
    low = lax.broadcasted_iota(jnp.int32, (1, 128), 1) < 64
    scales = (
        jnp.where(low, 0.125, 0.0).astype(jnp.bfloat16),
        jnp.where(low, 0.0, 0.125).astype(jnp.bfloat16),
    )
    ones = jnp.ones((length, 128), jnp.bfloat16)
    pieces = [(column, row) for column in range(0, model, 128) for row in range(0, length, block)]
    share = length // len(pieces)
    for part, (column, row) in enumerate(pieces):
        for r in range(part * share, (part + 1) * share):
            emb_ref[later, pl.ds(r, 1)] = wide_ref[pl.ds(place_ref[following, 0, r], 1)]
        query = qkv_ref[row : row + block, column : column + 128]
        keys = qkv_ref[:, model + column : model + column + 128]
        values = qkv_ref[:, 2 * model + column : 2 * model + column + 128]
        values = jnp.concatenate([values, ones], axis=1)
        heads = []
        for scale in scales:
            scores = lax.dot_general(
                query * scale, keys, (((1,), (1,)), ((), ())), preferred_element_type=jnp.float32
            )
            top = jnp.max(scores, axis=-1, keepdims=True)
            weights = jnp.exp(scores - top).astype(jnp.bfloat16)
            heads.append(jnp.dot(weights, values, preferred_element_type=jnp.float32))
        sums = jnp.where(low, heads[0][:, 128:], heads[1][:, 128:])
        mixed = jnp.where(low, heads[0][:, :128], heads[1][:, :128]) / sums
        mixed_ref[row : row + block, column : column + 128] = mixed.astype(jnp.bfloat16)
    resid = resid + jnp.dot(mixed_ref[...], w_out_ref[...], preferred_element_type=jnp.float32)
    normed = layer_norm(resid, gains_ref[1:2, :]).astype(jnp.bfloat16)
    inner = jax.nn.gelu(
        jnp.dot(normed, w_up_ref[...], preferred_element_type=jnp.float32)
    ).astype(jnp.bfloat16)
    resid = resid + jnp.dot(inner, w_down_ref[...], preferred_element_type=jnp.float32)
    final = layer_norm(resid, final_ref[...])
    logits = jnp.sum(final * score_ref[...].astype(jnp.float32), axis=-1).reshape(1, length)
    shifted = logits - jnp.max(logits, axis=-1, keepdims=True)
    total = jnp.sum(jnp.exp(shifted), axis=-1, keepdims=True)
    out_ref[...] = (shifted - jnp.log(total))[None]


def score_slates(rows, place, w_in, w_qkv, w_out, w_up, w_down, norm_gains, final_gain, w_score):
    slates, _, length = place.shape
    model = w_in.shape[1]
    whole = (
        rows, w_in, w_qkv[0], w_out[0], w_up[0], w_down[0], norm_gains[0], final_gain[None],
        w_score[None],
    )
    scored = pl.pallas_call(
        functools.partial(slate_kernel, block=128),
        grid=(slates,),
        in_specs=[pl.BlockSpec(memory_space=pltpu.SMEM)]
        + [pl.BlockSpec(a.shape, lambda i: (0, 0)) for a in whole],
        out_specs=pl.BlockSpec((1, 1, length), lambda i: (i, 0, 0)),
        out_shape=jax.ShapeDtypeStruct((slates, 1, length), jnp.float32),
        scratch_shapes=[
            pltpu.VMEM((length, 3 * model), jnp.bfloat16),
            pltpu.VMEM((length, model), jnp.bfloat16),
            pltpu.VMEM(rows.shape, jnp.float32),
            pltpu.VMEM((2, length, rows.shape[1]), jnp.float32),
        ],
        compiler_params=pltpu.CompilerParams(vmem_limit_bytes=40 * 1024 * 1024),
        name="slates",
    )(place, *whole)
    return scored.reshape(slates, length)


def hops(move):
    return sum(min(part, 4 - part) for part in move[:3])


MOVES = sorted(
    ((x, y, z, c) for x in range(4) for y in range(4) for z in range(4) for c in range(2)),
    key=lambda move: -hops(move),
)[:-2] + [(0, 0, 0, 1)]


def number_kernel(owner_ref, row_ref, want_ref, place_ref, sums, flat, before, lower, *, shards, capacity):
    slates, _, slate = owner_ref.shape
    lower[...] = (
        lax.broadcasted_iota(jnp.int32, (slate, slate), 0)
        <= lax.broadcasted_iota(jnp.int32, (slate, slate), 1)
    ).astype(jnp.bfloat16)
    before[...] = jnp.zeros_like(before)
    sums[...] = jnp.zeros_like(sums)

    def number(s, carry):
        owner, row = owner_ref[s], row_ref[pl.ds(s, 1), :]
        own = lax.broadcasted_iota(jnp.int32, (shards, slate), 0) == owner
        onehot = own.astype(jnp.float32).astype(jnp.bfloat16)
        within = jnp.dot(onehot, lower[...], preferred_element_type=jnp.float32)
        count = jnp.sum(jnp.where(own, within + before[...], 0.0), axis=0, keepdims=True)
        slot = (count - 1.0).astype(jnp.int32)
        before[...] += within[:, slate - 1 :]
        place_ref[s] = owner * capacity + slot
        pick = lax.broadcasted_iota(jnp.int32, (capacity, slate), 0) == slot
        low, high = (row & 255).astype(jnp.float32), ((row >> 8) - 128).astype(jnp.float32)
        halves = jnp.concatenate([jnp.where(pick, low, 0.0), jnp.where(pick, high, 0.0)], axis=0)
        sums[...] += lax.dot_general(
            onehot, halves.astype(jnp.bfloat16), (((1,), (1,)), ((), ())),
            preferred_element_type=jnp.float32,
        )
        return carry

    lax.fori_loop(0, slates, number, 0)
    both = sums[...]
    flat[...] = (both + 256.0 * pltpu.roll(both, capacity, 1)).astype(jnp.int32) + 32768
    for shard in range(shards):
        want_ref[shard] = flat[shard : shard + 1, :]


def number_candidates(owner, row, shards, capacity):
    slates, _, slate = owner.shape
    lanes = 2 * capacity
    whole = pl.BlockSpec(memory_space=pltpu.VMEM)
    return pl.pallas_call(
        functools.partial(number_kernel, shards=shards, capacity=capacity),
        in_specs=[whole, whole],
        out_specs=(whole, whole),
        out_shape=(
            jax.ShapeDtypeStruct((shards, 1, lanes), jnp.int32),
            jax.ShapeDtypeStruct((slates, 1, slate), jnp.int32),
        ),
        scratch_shapes=[
            pltpu.VMEM((shards, lanes), jnp.float32),
            pltpu.VMEM((shards, lanes), jnp.int32),
            pltpu.VMEM((shards, 1), jnp.float32),
            pltpu.VMEM((slate, slate), jnp.bfloat16),
        ],
        compiler_params=pltpu.CompilerParams(vmem_limit_bytes=4 * 1024 * 1024),
        name="number",
    )(owner, row)


def exchange_kernel(
    want_ref, table_ref, out_ref, packed, table, block, sending, asked, numbers,
    chunk_sems, ask_send, ask_recv, row_send, row_recv, number_sem, *, shards, chunks, early, capacity,
):
    length = table_ref.shape[0] // chunks
    ring = packed.shape[0] // length
    gx, gy = lax.axis_index("gx"), lax.axis_index("gy")
    me = gx * 4 + gy
    x, y, core = gx // 8, (gx // 2) % 4, gx % 2
    xs = [((x + d) % 4) * 8 for d in range(4)]
    ys = [((y + d) % 4) * 2 for d in range(4)]
    zs = [(gy + d) % 4 for d in range(4)]
    cores = [core, 1 - core]

    def peer(move):
        to_gx, to_gy = xs[move[0]] + ys[move[1]] + cores[move[3]], zs[move[2]]
        return to_gx, to_gy, to_gx * 4 + to_gy

    def chunk_copy(chunk):
        source = table_ref.at[pl.ds(chunk * length, length)]
        target = packed.at[pl.ds((chunk % ring) * length, length)]
        return pltpu.make_async_copy(source, target, chunk_sems.at[chunk % ring])

    def load(chunk):
        chunk_copy(chunk).wait()

        def widen(part, carry):
            piece = packed[pl.ds((chunk % ring) * length + part * 128, 128)]
            table[pl.ds(chunk * length + part * 128, 128)] = piece.astype(jnp.float32)
            return carry

        lax.fori_loop(0, length // 128, widen, 0)
        if chunk + ring < chunks:
            chunk_copy(chunk + ring).start()

    for chunk in range(ring):
        chunk_copy(chunk).start()
    barrier = pltpu.get_barrier_semaphore()
    for move in MOVES:
        to_gx, to_gy, _ = peer(move)
        pl.semaphore_signal(barrier, inc=1, device_id=(to_gx, to_gy), device_id_type=MESH)
    for chunk in range(early):
        load(chunk)
    pl.semaphore_wait(barrier, shards - 1)
    for move in MOVES:
        to_gx, to_gy, shard = peer(move)
        pltpu.make_async_remote_copy(
            src_ref=want_ref.at[shard], dst_ref=asked.at[me], send_sem=ask_send, recv_sem=ask_recv,
            device_id=(to_gx, to_gy), device_id_type=MESH,
        ).start()
    asked[pl.ds(me, 1)] = want_ref[pl.ds(me, 1)]
    for chunk in range(early, chunks):
        load(chunk)
    others = pl.ds(0, shards - 1)
    pltpu.make_async_copy(asked.at[others], asked.at[others], ask_recv).wait()
    pltpu.make_async_copy(asked.at[others], asked.at[others], ask_send).wait()
    copy = pltpu.make_async_copy(asked, numbers, number_sem)
    copy.start()
    copy.wait()

    def collect(shard, target):
        for slot in range(capacity):
            block[pl.ds(slot, 1)] = table[pl.ds(numbers[shard, 0, slot], 1)]
        target[...] = block[...].astype(jnp.bfloat16)

    def receiver(step):
        a, b, c = step % 4, (step // 8) % 4, (step // 32) % 4
        to_gx = ((x + a) % 4) * 8 + ((y + a + b) % 4) * 2 + (core + (step // 4) % 2) % 2
        to_gy = (gy + a + c) % 4
        return to_gx, to_gy, to_gx * 4 + to_gy

    def send(step):
        to_gx, to_gy, shard = receiver(step)
        pltpu.make_async_remote_copy(
            src_ref=sending.at[shard], dst_ref=out_ref.at[me], send_sem=row_send, recv_sem=row_recv,
            device_id=(to_gx, to_gy), device_id_type=MESH,
        ).start()

    def give(step, carry):
        shard = receiver(step)[2]
        collect(shard, sending.at[shard])
        pl.when(step > 1)(lambda: send(step - 1))
        return carry

    lax.fori_loop(1, shards, give, 0)
    collect(me, out_ref.at[me])
    send(shards - 1)
    pltpu.make_async_copy(out_ref.at[others], out_ref.at[others], row_recv).wait()
    pltpu.make_async_copy(out_ref.at[others], out_ref.at[others], row_send).wait()


def exchange(want, item_table, capacity):
    shards, _, lanes = want.shape
    rows, width = item_table.shape
    chunks, ring, early = 12, 4, 4
    whole = pl.BlockSpec(memory_space=pltpu.VMEM)
    return pl.pallas_call(
        functools.partial(
            exchange_kernel, shards=shards, chunks=chunks, early=early, capacity=capacity
        ),
        in_specs=[whole, pl.BlockSpec(memory_space=pl.ANY)],
        out_specs=whole,
        out_shape=jax.ShapeDtypeStruct((shards, capacity, width), jnp.bfloat16),
        scratch_shapes=[
            pltpu.VMEM((rows // chunks * ring, width), jnp.bfloat16),
            pltpu.VMEM((rows, width), jnp.float32),
            pltpu.VMEM((capacity, width), jnp.float32),
            pltpu.VMEM((shards, capacity, width), jnp.bfloat16),
            pltpu.VMEM((shards, 1, lanes), jnp.int32),
            pltpu.SMEM((shards, 1, lanes), jnp.int32),
            pltpu.SemaphoreType.DMA((ring,)),
        ]
        + [pltpu.SemaphoreType.DMA] * 5,
        compiler_params=pltpu.CompilerParams(
            collective_id=0, has_side_effects=True, vmem_limit_bytes=52 * 1024 * 1024
        ),
        name="exchange",
    )(want, item_table)


def per_device(
    candidate_owner,
    candidate_row,
    item_table,
    w_in,
    w_qkv,
    w_out,
    w_up,
    w_down,
    norm_gains,
    final_gain,
    w_score,
):
    slates, length, unused = candidate_owner.shape
    width = item_table.shape[1]
    shards = lax.axis_size(("gx", "gy"))
    capacity = max(2, 2 * slates * length // shards)
    want, place = number_candidates(
        candidate_owner.reshape(slates, 1, length), candidate_row, shards, capacity
    )
    rows = exchange(want, item_table, capacity)
    rows = rows.reshape(shards * capacity, width)
    return score_slates(
        rows, place, w_in, w_qkv, w_out, w_up, w_down, norm_gains, final_gain, w_score
    )


def solution(mesh):
    return jax.shard_map(
        per_device,
        mesh=mesh,
        in_specs=(
            P(("gx", "gy"), None, None),
            P(("gx", "gy"), None),
            P(("gx", "gy"), None),
            P(),
            P(),
            P(),
            P(),
            P(),
            P(),
            P(),
            P(),
        ),
        out_specs=P(("gx", "gy"), None),
        check_vma=False,
    )
```

```python
import functools

import jax
import jax.numpy as jnp
from jax import lax
from jax.experimental import pallas as pl
from jax.experimental.pallas import tpu as pltpu
from jax.sharding import PartitionSpec as P

MESH = pl.DeviceIdType.MESH
TOGETHER = 2


def layer_norm(values, gain):
    mean = jnp.mean(values, axis=-1, keepdims=True)
    centred = values - mean
    variance = jnp.mean(centred * centred, axis=-1, keepdims=True)
    return centred * lax.rsqrt(variance + 1e-05) * gain


def slate_kernel(
    place_ref, rows_ref, w_in_ref, w_qkv_ref, w_out_ref, w_up_ref, w_down_ref, gains_ref, final_ref,
    score_ref, out_ref, resid_ref, qkv_ref, mixed_ref, packed_ref, wide_ref, emb_ref, piece_sems, *, block,
):
    together, length, model = mixed_ref.shape
    slates = range(together)
    step = pl.program_id(0)
    now, later = step % 2, (step + 1) % 2
    following = jnp.minimum(step + 1, pl.num_programs(0) - 1) * together

    @pl.when(step == 0)
    def _():
        pieces = piece_sems.shape[0]
        count = rows_ref.shape[0] // pieces
        copies = [
            pltpu.make_async_copy(
                rows_ref.at[pl.ds(p * count, count)], packed_ref.at[pl.ds(p * count, count)], piece_sems.at[p]
            )
            for p in range(pieces)
        ]
        for copy in copies:
            copy.start()
        for p, copy in enumerate(copies):
            copy.wait()

            def widen(part, carry):
                piece = pl.ds(pl.multiple_of(p * count + part * 256, 256), 256)
                wide_ref[piece] = packed_ref[piece].astype(jnp.float32)
                return carry

            lax.fori_loop(0, count // 256, widen, 0)

        def fetch(part, carry):
            first = pl.multiple_of(part * 32, 32)
            for s in slates:
                for r in range(32):
                    row = wide_ref[pl.ds(place_ref[s, 0, first + r], 1)]
                    emb_ref[0, s, pl.ds(first + r, 1)] = row
            return carry

        lax.fori_loop(0, length // 32, fetch, 0)

    def matmul(values, weights_ref):
        return jnp.dot(values, weights_ref[...], preferred_element_type=jnp.float32)

    def add_resid(s, values):
        total = resid_ref[s] + values
        resid_ref[s] = total
        return total

    def beside(first, second, values):
        results, held = [], None
        for s in slates:
            passed = first(s, values[s])
            if s:
                results.append(second(s - 1, held))
            held = passed
        return results + [second(together - 1, held)]

    def project(s, normed):
        qkv_ref[s] = matmul(normed, w_qkv_ref).astype(jnp.bfloat16)

    def start(s):
        resid_ref[s] = matmul(emb_ref[now, s].astype(jnp.bfloat16), w_in_ref)
        return resid_ref[s]

    def normalise(row):
        gain = gains_ref[row : row + 1, :]
        return lambda s, values: layer_norm(values, gain).astype(jnp.bfloat16)

    beside(normalise(0), project, [start(s) for s in slates])

    low = lax.broadcasted_iota(jnp.int32, (1, 128), 1) < 64
    scales = (
        jnp.where(low, 0.125, 0.0).astype(jnp.bfloat16),
        jnp.where(low, 0.0, 0.125).astype(jnp.bfloat16),
    )
    ones = jnp.ones((length, 128), jnp.bfloat16)
    pieces = [
        (s, column, row)
        for column in range(0, model, 128)
        for s in slates
        for row in range(0, length, block)
    ]
    share = together * length // len(pieces)
    for part, (s, column, row) in enumerate(pieces):
        for r in range(part * share, (part + 1) * share):
            ahead, r = divmod(r, length)
            fetched = wide_ref[pl.ds(place_ref[following + ahead, 0, r], 1)]
            emb_ref[later, ahead, pl.ds(r, 1)] = fetched
        query = qkv_ref[s, row : row + block, column : column + 128]
        keys = qkv_ref[s, :, model + column : model + column + 128]
        values = qkv_ref[s, :, 2 * model + column : 2 * model + column + 128]
        values = jnp.concatenate([values, ones], axis=1)
        heads = []
        for scale in scales:
            scores = lax.dot_general(
                query * scale, keys, (((1,), (1,)), ((), ())), preferred_element_type=jnp.float32
            )
            top = jnp.max(scores, axis=-1, keepdims=True)
            weights = jnp.exp(scores - top).astype(jnp.bfloat16)
            heads.append(jnp.dot(weights, values, preferred_element_type=jnp.float32))
        sums = jnp.where(low, heads[0][:, 128:], heads[1][:, 128:])
        mixed = jnp.where(low, heads[0][:, :128], heads[1][:, :128]) / sums
        mixed_ref[s, row : row + block, column : column + 128] = mixed.astype(jnp.bfloat16)

    resid = [add_resid(s, matmul(mixed_ref[s], w_out_ref)) for s in slates]
    raised = beside(normalise(1), lambda s, normed: matmul(normed, w_up_ref), resid)
    lowered = beside(
        lambda s, values: jax.nn.gelu(values).astype(jnp.bfloat16),
        lambda s, inner: matmul(inner, w_down_ref),
        raised,
    )
    for s in slates:
        final = layer_norm(resid_ref[s] + lowered[s], final_ref[...])
        logits = jnp.sum(final * score_ref[...].astype(jnp.float32), axis=-1).reshape(1, length)
        shifted = logits - jnp.max(logits, axis=-1, keepdims=True)
        total = jnp.sum(jnp.exp(shifted), axis=-1, keepdims=True)
        out_ref[s] = shifted - jnp.log(total)


def score_slates(rows, place, w_in, w_qkv, w_out, w_up, w_down, norm_gains, final_gain, w_score):
    slates, _, length = place.shape
    model = w_in.shape[1]
    together = TOGETHER
    whole = (
        rows, w_in, w_qkv[0], w_out[0], w_up[0], w_down[0], norm_gains[0], final_gain[None],
        w_score[None],
    )
    scored = pl.pallas_call(
        functools.partial(slate_kernel, block=128),
        grid=(slates // together,),
        in_specs=[pl.BlockSpec(memory_space=pltpu.SMEM), pl.BlockSpec(memory_space=pl.ANY)]
        + [pl.BlockSpec(a.shape, lambda i: (0, 0)) for a in whole[1:]],
        out_specs=pl.BlockSpec((together, 1, length), lambda i: (i, 0, 0)),
        out_shape=jax.ShapeDtypeStruct((slates, 1, length), jnp.float32),
        scratch_shapes=[
            pltpu.VMEM((together, length, model), jnp.float32),
            pltpu.VMEM((together, length, 3 * model), jnp.bfloat16),
            pltpu.VMEM((together, length, model), jnp.bfloat16),
            pltpu.VMEM(rows.shape, jnp.bfloat16),
            pltpu.VMEM(rows.shape, jnp.float32),
            pltpu.VMEM((2, together, length, rows.shape[1]), jnp.float32),
            pltpu.SemaphoreType.DMA((8,)),
        ],
        compiler_params=pltpu.CompilerParams(vmem_limit_bytes=48 * 1024 * 1024),
        name="slates",
    )(place, *whole)
    return scored.reshape(slates, length)


def hops(move):
    return sum(min(part, 4 - part) for part in move[:3])


def move_of(group, member):
    a = member % 4
    return a, (a + group[0]) % 4, (a + group[1]) % 4, member // 4


MEMBERS = 8
GROUPS = sorted(
    ((b, c) for b in range(4) for c in range(4)),
    key=lambda group: max(hops(move_of(group, member)) for member in range(MEMBERS)),
)
GROUPS = GROUPS[:6] + GROUPS[:5:-1]
MOVES = [(group, member) for group in GROUPS for member in range(MEMBERS)]
MOVES.remove(((0, 0), 0))


def back(group, member):
    return GROUPS.index((-group[0] % 4, -group[1] % 4)), -member % 4 + member // 4 * 4


def number_kernel(owner_ref, row_ref, want_ref, place_ref, flat, lower, *, shards, capacity):
    slates, _, slate = owner_ref.shape
    lower[...] = (
        lax.broadcasted_iota(jnp.int32, (slate, slate), 0)
        <= lax.broadcasted_iota(jnp.int32, (slate, slate), 1)
    ).astype(jnp.bfloat16)
    seen = jnp.zeros((shards, 1), jnp.float32)
    both = jnp.zeros((shards, 2 * capacity), jnp.float32)
    for s in range(slates):
        owner, row = owner_ref[s], row_ref[s : s + 1, :]
        own = lax.broadcasted_iota(jnp.int32, (shards, slate), 0) == owner
        onehot = own.astype(jnp.float32).astype(jnp.bfloat16)
        within = jnp.dot(onehot, lower[...], preferred_element_type=jnp.float32)
        count = jnp.sum(jnp.where(own, within + seen, 0.0), axis=0, keepdims=True)
        slot = (count - 1.0).astype(jnp.int32)
        seen = seen + within[:, slate - 1 :]
        place_ref[s] = owner * capacity + slot
        pick = lax.broadcasted_iota(jnp.int32, (capacity, slate), 0) == slot
        low, high = (row & 255).astype(jnp.float32), ((row >> 8) - 128).astype(jnp.float32)
        halves = jnp.concatenate([jnp.where(pick, low, 0.0), jnp.where(pick, high, 0.0)], axis=0)
        both = both + lax.dot_general(
            onehot, halves.astype(jnp.bfloat16), (((1,), (1,)), ((), ())),
            preferred_element_type=jnp.float32,
        )
    flat[...] = (both + 256.0 * pltpu.roll(both, capacity, 1)).astype(jnp.int32) + 32768
    for shard in range(shards):
        want_ref[shard] = flat[shard : shard + 1, :]


def number_candidates(owner, row, shards, capacity):
    slates, _, slate = owner.shape
    lanes = 2 * capacity
    whole = pl.BlockSpec(memory_space=pltpu.VMEM)
    return pl.pallas_call(
        functools.partial(number_kernel, shards=shards, capacity=capacity),
        in_specs=[whole, whole],
        out_specs=(whole, whole),
        out_shape=(
            jax.ShapeDtypeStruct((shards, 1, lanes), jnp.int32),
            jax.ShapeDtypeStruct((slates, 1, slate), jnp.int32),
        ),
        scratch_shapes=[
            pltpu.VMEM((shards, lanes), jnp.int32),
            pltpu.VMEM((slate, slate), jnp.bfloat16),
        ],
        compiler_params=pltpu.CompilerParams(vmem_limit_bytes=8 * 1024 * 1024),
        name="number",
    )(owner, row)


def exchange_kernel(
    want_ref, table_ref, out_ref, packed, table, block, sending, asked, numbers,
    chunk_sems, ask_send, ask_recv, row_send, row_recv, number_sems, own_sem,
    *, shards, chunks, early, capacity,
):
    length = table_ref.shape[0] // chunks
    ring = packed.shape[0] // length
    gx, gy = lax.axis_index("gx"), lax.axis_index("gy")
    me = gx * 4 + gy
    x, y, core = gx // 8, (gx // 2) % 4, gx % 2
    xs = [((x + d) % 4) * 8 for d in range(4)]
    ys = [((y + d) % 4) * 2 for d in range(4)]
    zs = [(gy + d) % 4 for d in range(4)]
    cores = [core, 1 - core]

    def peer(move):
        to_gx, to_gy = xs[move[0]] + ys[move[1]] + cores[move[3]], zs[move[2]]
        return to_gx, to_gy, to_gx * 4 + to_gy

    def chunk_copy(chunk):
        source = table_ref.at[pl.ds(chunk * length, length)]
        target = packed.at[pl.ds((chunk % ring) * length, length)]
        return pltpu.make_async_copy(source, target, chunk_sems.at[chunk % ring])

    def load(chunk):
        chunk_copy(chunk).wait()

        def widen(part, carry):
            piece = packed[pl.ds((chunk % ring) * length + part * 128, 128)]
            table[pl.ds(chunk * length + part * 128, 128)] = piece.astype(jnp.float32)
            return carry

        lax.fori_loop(0, length // 128, widen, 0)
        if chunk + ring < chunks:
            chunk_copy(chunk + ring).start()

    for chunk in range(ring):
        chunk_copy(chunk).start()
    barrier = pltpu.get_barrier_semaphore()
    for group, member in reversed(MOVES):
        to_gx, to_gy, _ = peer(move_of(group, member))
        pl.semaphore_signal(barrier, inc=1, device_id=(to_gx, to_gy), device_id_type=MESH)
    for chunk in range(early):
        load(chunk)
    pl.semaphore_wait(barrier, shards - 1)
    for group, member in sorted(MOVES, key=lambda move: back(*move)):
        to_gx, to_gy, shard = peer(move_of(group, member))
        there, place = back(group, member)
        pltpu.make_async_remote_copy(
            src_ref=want_ref.at[shard], dst_ref=asked.at[there * MEMBERS + place],
            send_sem=ask_send, recv_sem=ask_recv.at[there],
            device_id=(to_gx, to_gy), device_id_type=MESH,
        ).start()
    home = GROUPS.index((0, 0))
    asked[pl.ds(home * MEMBERS, 1)] = want_ref[pl.ds(me, 1)]
    for chunk in range(early, chunks):
        load(chunk)

    def number_copy(number):
        members = pl.ds(number * MEMBERS, MEMBERS)
        return pltpu.make_async_copy(asked.at[members], numbers.at[members], number_sems.at[number])

    def hear(number):
        heard = pl.ds(number * MEMBERS, MEMBERS)
        if number == home:
            heard = pl.ds(number * MEMBERS + 1, MEMBERS - 1)
        pltpu.make_async_copy(asked.at[heard], asked.at[heard], ask_recv.at[number]).wait()
        number_copy(number).start()

    def collect(place, shard):
        for slot in range(capacity):
            block[pl.ds(slot, 1)] = table[pl.ds(numbers[place, 0, slot], 1)]
        sending[shard] = block[...].astype(jnp.bfloat16)

    def receiver(group, member):
        a = member % 4
        to_gx = ((x + a) % 4) * 8 + ((y + a + group[0]) % 4) * 2 + (core + member // 4) % 2
        to_gy = (gy + a + group[1]) % 4
        return to_gx, to_gy, to_gx * 4 + to_gy

    def send(group, member):
        to_gx, to_gy, shard = receiver(group, member)
        pltpu.make_async_remote_copy(
            src_ref=sending.at[shard], dst_ref=out_ref.at[me], send_sem=row_send, recv_sem=row_recv,
            device_id=(to_gx, to_gy), device_id_type=MESH,
        ).start()

    hear(0)
    for number, group in enumerate(GROUPS):
        if number + 1 < len(GROUPS):
            hear(number + 1)
        number_copy(number).wait()
        if number:
            send(GROUPS[number - 1], MEMBERS - 1)
        first = 1 if number == home else 0

        def give(member, carry):
            collect(number * MEMBERS + member, receiver(group, member)[2])
            pl.when(member > first)(lambda: send(group, member - 1))
            return carry

        lax.fori_loop(first, MEMBERS, give, 0)
    collect(home * MEMBERS, me)
    send(GROUPS[-1], MEMBERS - 1)
    others = pl.ds(0, shards - 1)
    pltpu.make_async_copy(asked.at[others], asked.at[others], ask_send).wait()
    own = pltpu.make_async_copy(sending.at[me], out_ref.at[me], own_sem)
    own.start()
    own.wait()
    pltpu.make_async_copy(sending.at[others], sending.at[others], row_recv).wait()
    pltpu.make_async_copy(sending.at[others], sending.at[others], row_send).wait()


def exchange(want, item_table, capacity):
    shards, _, lanes = want.shape
    rows, width = item_table.shape
    chunks, ring, early = 12, 4, 6
    whole, anywhere = pl.BlockSpec(memory_space=pltpu.VMEM), pl.BlockSpec(memory_space=pl.ANY)
    return pl.pallas_call(
        functools.partial(
            exchange_kernel, shards=shards, chunks=chunks, early=early, capacity=capacity
        ),
        in_specs=[whole, anywhere],
        out_specs=anywhere,
        out_shape=jax.ShapeDtypeStruct((shards, capacity, width), jnp.bfloat16),
        scratch_shapes=[
            pltpu.VMEM((rows // chunks * ring, width), jnp.bfloat16),
            pltpu.VMEM((rows, width), jnp.float32),
            pltpu.VMEM((capacity, width), jnp.float32),
            pltpu.VMEM((shards, capacity, width), jnp.bfloat16),
            pltpu.VMEM((shards, 1, lanes), jnp.int32),
            pltpu.SMEM((shards, 1, lanes), jnp.int32),
            pltpu.SemaphoreType.DMA((ring,)),
            pltpu.SemaphoreType.DMA,
            pltpu.SemaphoreType.DMA((len(GROUPS),)),
            pltpu.SemaphoreType.DMA,
            pltpu.SemaphoreType.DMA,
            pltpu.SemaphoreType.DMA((len(GROUPS),)),
            pltpu.SemaphoreType.DMA,
        ],
        compiler_params=pltpu.CompilerParams(
            collective_id=0, has_side_effects=True, vmem_limit_bytes=52 * 1024 * 1024
        ),
        name="exchange",
    )(want, item_table)


def per_device(
    candidate_owner,
    candidate_row,
    item_table,
    w_in,
    w_qkv,
    w_out,
    w_up,
    w_down,
    norm_gains,
    final_gain,
    w_score,
):
    slates, length, unused = candidate_owner.shape
    width = item_table.shape[1]
    shards = lax.axis_size(("gx", "gy"))
    capacity = max(2, 2 * slates * length // shards)
    want, place = number_candidates(
        candidate_owner.reshape(slates, 1, length), candidate_row, shards, capacity
    )
    rows = exchange(want, item_table, capacity)
    rows = rows.reshape(shards * capacity, width)
    return score_slates(
        rows, place, w_in, w_qkv, w_out, w_up, w_down, norm_gains, final_gain, w_score
    )


def solution(mesh):
    return jax.shard_map(
        per_device,
        mesh=mesh,
        in_specs=(
            P(("gx", "gy"), None, None),
            P(("gx", "gy"), None),
            P(("gx", "gy"), None),
            P(),
            P(),
            P(),
            P(),
            P(),
            P(),
            P(),
            P(),
        ),
        out_specs=P(("gx", "gy"), None),
        check_vma=False,
    )
```

```python
import functools

import jax
import jax.numpy as jnp
from jax import lax
from jax.experimental import pallas as pl
from jax.experimental.pallas import tpu as pltpu
from jax.sharding import PartitionSpec as P

MESH = pl.DeviceIdType.MESH
TOGETHER = 4


def layer_norm(values, gain):
    mean = jnp.mean(values, axis=-1, keepdims=True)
    centred = values - mean
    variance = jnp.mean(centred * centred, axis=-1, keepdims=True)
    return centred * lax.rsqrt(variance + 1e-05) * gain


def slate_kernel(
    place_ref, rows_ref, w_in_ref, w_qkv_ref, w_out_ref, w_up_ref, w_down_ref, gains_ref, final_ref,
    score_ref, out_ref, resid_ref, qkv_ref, mixed_ref, packed_ref, wide_ref, emb_ref, piece_sems, *, block,
):
    together, length, model = mixed_ref.shape
    slates = range(together)
    step = pl.program_id(0)
    now, later = step % 2, (step + 1) % 2
    following = jnp.minimum(step + 1, pl.num_programs(0) - 1) * together

    @pl.when(step == 0)
    def _():
        pieces = piece_sems.shape[0]
        count = rows_ref.shape[0] // pieces
        copies = [
            pltpu.make_async_copy(
                rows_ref.at[pl.ds(p * count, count)], packed_ref.at[pl.ds(p * count, count)], piece_sems.at[p]
            )
            for p in range(pieces)
        ]
        for copy in copies:
            copy.start()
        for p, copy in enumerate(copies):
            copy.wait()

            def widen(part, carry):
                piece = pl.ds(pl.multiple_of(p * count + part * 256, 256), 256)
                wide_ref[piece] = packed_ref[piece].astype(jnp.float32)
                return carry

            lax.fori_loop(0, count // 256, widen, 0)

        def fetch(part, carry):
            first = pl.multiple_of(part * 32, 32)
            for r in range(32):
                row = wide_ref[pl.ds(place_ref[0, 0, first + r], 1)]
                emb_ref[0, 0, pl.ds(first + r, 1)] = row
            return carry

        lax.fori_loop(0, length // 32, fetch, 0)

    def matmul(values, weights_ref):
        return jnp.dot(values, weights_ref[...], preferred_element_type=jnp.float32)

    def add_resid(s, values):
        total = resid_ref[s] + values
        resid_ref[s] = total
        return total

    def beside(first, second, values):
        results, held = [], None
        for s in slates:
            passed = first(s, values[s])
            if s:
                results.append(second(s - 1, held))
            held = passed
        return results + [second(together - 1, held)]

    def project(s, normed):
        qkv_ref[s] = matmul(normed, w_qkv_ref).astype(jnp.bfloat16)

    def start(s):
        if s:
            for r in range(length):
                row = wide_ref[pl.ds(place_ref[step * together + s, 0, r], 1)]
                emb_ref[now, s, pl.ds(r, 1)] = row
        resid_ref[s] = matmul(emb_ref[now, s].astype(jnp.bfloat16), w_in_ref)
        return resid_ref[s]

    def normalise(row):
        gain = gains_ref[row : row + 1, :]
        return lambda s, values: layer_norm(values, gain).astype(jnp.bfloat16)

    first_norm = normalise(0)
    beside(lambda s, _: first_norm(s, start(s)), project, [None] * together)

    low = lax.broadcasted_iota(jnp.int32, (1, 128), 1) < 64
    scales = (
        jnp.where(low, 0.125, 0.0).astype(jnp.bfloat16),
        jnp.where(low, 0.0, 0.125).astype(jnp.bfloat16),
    )
    ones = jnp.ones((length, 128), jnp.bfloat16)
    pieces = [
        (s, column, row)
        for column in range(0, model, 128)
        for s in slates
        for row in range(0, length, block)
    ]
    share = length // len(pieces)
    for part, (s, column, row) in enumerate(pieces):
        for r in range(part * share, (part + 1) * share):
            ahead, r = divmod(r, length)
            fetched = wide_ref[pl.ds(place_ref[following + ahead, 0, r], 1)]
            emb_ref[later, ahead, pl.ds(r, 1)] = fetched
        query = qkv_ref[s, row : row + block, column : column + 128]
        keys = qkv_ref[s, :, model + column : model + column + 128]
        values = qkv_ref[s, :, 2 * model + column : 2 * model + column + 128]
        values = jnp.concatenate([values, ones], axis=1)
        heads = []
        for scale in scales:
            scores = lax.dot_general(
                query * scale, keys, (((1,), (1,)), ((), ())), preferred_element_type=jnp.float32
            )
            top = jnp.max(scores, axis=-1, keepdims=True)
            weights = jnp.exp(scores - top).astype(jnp.bfloat16)
            heads.append(jnp.dot(weights, values, preferred_element_type=jnp.float32))
        sums = jnp.where(low, heads[0][:, 128:], heads[1][:, 128:])
        mixed = jnp.where(low, heads[0][:, :128], heads[1][:, :128]) / sums
        mixed_ref[s, row : row + block, column : column + 128] = mixed.astype(jnp.bfloat16)

    resid = [add_resid(s, matmul(mixed_ref[s], w_out_ref)) for s in slates]
    raised = beside(normalise(1), lambda s, normed: matmul(normed, w_up_ref), resid)
    lowered = beside(
        lambda s, values: jax.nn.gelu(values).astype(jnp.bfloat16),
        lambda s, inner: matmul(inner, w_down_ref),
        raised,
    )
    for s in slates:
        final = layer_norm(resid_ref[s] + lowered[s], final_ref[...])
        logits = jnp.sum(final * score_ref[...].astype(jnp.float32), axis=-1).reshape(1, length)
        shifted = logits - jnp.max(logits, axis=-1, keepdims=True)
        total = jnp.sum(jnp.exp(shifted), axis=-1, keepdims=True)
        out_ref[s] = shifted - jnp.log(total)


def score_slates(rows, place, w_in, w_qkv, w_out, w_up, w_down, norm_gains, final_gain, w_score):
    slates, _, length = place.shape
    model = w_in.shape[1]
    together = TOGETHER
    whole = (
        rows, w_in, w_qkv[0], w_out[0], w_up[0], w_down[0], norm_gains[0], final_gain[None],
        w_score[None],
    )
    scored = pl.pallas_call(
        functools.partial(slate_kernel, block=128),
        grid=(slates // together,),
        in_specs=[pl.BlockSpec(memory_space=pltpu.SMEM), pl.BlockSpec(memory_space=pl.ANY)]
        + [pl.BlockSpec(a.shape, lambda i: (0, 0)) for a in whole[1:]],
        out_specs=pl.BlockSpec((together, 1, length), lambda i: (i, 0, 0)),
        out_shape=jax.ShapeDtypeStruct((slates, 1, length), jnp.float32),
        scratch_shapes=[
            pltpu.VMEM((together, length, model), jnp.float32),
            pltpu.VMEM((together, length, 3 * model), jnp.bfloat16),
            pltpu.VMEM((together, length, model), jnp.bfloat16),
            pltpu.VMEM(rows.shape, jnp.bfloat16),
            pltpu.VMEM(rows.shape, jnp.float32),
            pltpu.VMEM((2, together, length, rows.shape[1]), jnp.float32),
            pltpu.SemaphoreType.DMA((8,)),
        ],
        compiler_params=pltpu.CompilerParams(vmem_limit_bytes=48 * 1024 * 1024),
        name="slates",
    )(place, *whole)
    return scored.reshape(slates, length)


def hops(move):
    return sum(min(part, 4 - part) for part in move[:3])


def move_of(group, member):
    a = member % 4
    return a, (a + group[0]) % 4, (a + group[1]) % 4, member // 4


MEMBERS = 8
GROUPS = sorted(
    ((b, c) for b in range(4) for c in range(4)),
    key=lambda group: max(hops(move_of(group, member)) for member in range(MEMBERS)),
)
GROUPS = GROUPS[:6] + GROUPS[:5:-1]
MOVES = [(group, member) for group in GROUPS for member in range(MEMBERS)]
MOVES.remove(((0, 0), 0))


def back(group, member):
    return GROUPS.index((-group[0] % 4, -group[1] % 4)), -member % 4 + member // 4 * 4


def number_kernel(owner_ref, row_ref, want_ref, place_ref, flat, lower, *, shards, capacity):
    slates, _, slate = owner_ref.shape
    lower[...] = (
        lax.broadcasted_iota(jnp.int32, (slate, slate), 0)
        <= lax.broadcasted_iota(jnp.int32, (slate, slate), 1)
    ).astype(jnp.bfloat16)
    seen = jnp.zeros((shards, 1), jnp.float32)
    both = jnp.zeros((shards, 2 * capacity), jnp.float32)
    for s in range(slates):
        owner, row = owner_ref[s], row_ref[s : s + 1, :]
        own = lax.broadcasted_iota(jnp.int32, (shards, slate), 0) == owner
        onehot = own.astype(jnp.float32).astype(jnp.bfloat16)
        within = jnp.dot(onehot, lower[...], preferred_element_type=jnp.float32)
        count = jnp.sum(jnp.where(own, within + seen, 0.0), axis=0, keepdims=True)
        slot = (count - 1.0).astype(jnp.int32)
        seen = seen + within[:, slate - 1 :]
        place_ref[s] = owner * capacity + slot
        pick = lax.broadcasted_iota(jnp.int32, (capacity, slate), 0) == slot
        low, high = (row & 255).astype(jnp.float32), ((row >> 8) - 128).astype(jnp.float32)
        halves = jnp.concatenate([jnp.where(pick, low, 0.0), jnp.where(pick, high, 0.0)], axis=0)
        both = both + lax.dot_general(
            onehot, halves.astype(jnp.bfloat16), (((1,), (1,)), ((), ())),
            preferred_element_type=jnp.float32,
        )
    flat[...] = (both + 256.0 * pltpu.roll(both, capacity, 1)).astype(jnp.int32) + 32768
    for shard in range(shards):
        want_ref[shard] = flat[shard : shard + 1, :]


def number_candidates(owner, row, shards, capacity):
    slates, _, slate = owner.shape
    lanes = 2 * capacity
    whole = pl.BlockSpec(memory_space=pltpu.VMEM)
    return pl.pallas_call(
        functools.partial(number_kernel, shards=shards, capacity=capacity),
        in_specs=[whole, whole],
        out_specs=(whole, whole),
        out_shape=(
            jax.ShapeDtypeStruct((shards, 1, lanes), jnp.int32),
            jax.ShapeDtypeStruct((slates, 1, slate), jnp.int32),
        ),
        scratch_shapes=[
            pltpu.VMEM((shards, lanes), jnp.int32),
            pltpu.VMEM((slate, slate), jnp.bfloat16),
        ],
        compiler_params=pltpu.CompilerParams(vmem_limit_bytes=8 * 1024 * 1024),
        name="number",
    )(owner, row)


def exchange_kernel(
    want_ref, table_ref, out_ref, packed, table, block, sending, asked, numbers,
    chunk_sems, ask_send, ask_recv, row_send, row_recv, number_sems, own_sem,
    *, shards, chunks, early, capacity,
):
    length = table_ref.shape[0] // chunks
    ring = packed.shape[0] // length
    gx, gy = lax.axis_index("gx"), lax.axis_index("gy")
    me = gx * 4 + gy
    x, y, core = gx // 8, (gx // 2) % 4, gx % 2
    xs = [((x + d) % 4) * 8 for d in range(4)]
    ys = [((y + d) % 4) * 2 for d in range(4)]
    zs = [(gy + d) % 4 for d in range(4)]
    cores = [core, 1 - core]

    def peer(move):
        to_gx, to_gy = xs[move[0]] + ys[move[1]] + cores[move[3]], zs[move[2]]
        return to_gx, to_gy, to_gx * 4 + to_gy

    def chunk_copy(chunk):
        source = table_ref.at[pl.ds(chunk * length, length)]
        target = packed.at[pl.ds((chunk % ring) * length, length)]
        return pltpu.make_async_copy(source, target, chunk_sems.at[chunk % ring])

    def load(chunk):
        chunk_copy(chunk).wait()

        def widen(part, carry):
            piece = packed[pl.ds((chunk % ring) * length + part * 128, 128)]
            table[pl.ds(chunk * length + part * 128, 128)] = piece.astype(jnp.float32)
            return carry

        lax.fori_loop(0, length // 128, widen, 0)
        if chunk + ring < chunks:
            chunk_copy(chunk + ring).start()

    for chunk in range(ring):
        chunk_copy(chunk).start()
    barrier = pltpu.get_barrier_semaphore()
    for group, member in reversed(MOVES):
        to_gx, to_gy, _ = peer(move_of(group, member))
        pl.semaphore_signal(barrier, inc=1, device_id=(to_gx, to_gy), device_id_type=MESH)
    for chunk in range(early):
        load(chunk)
    pl.semaphore_wait(barrier, shards - 1)
    for group, member in sorted(MOVES, key=lambda move: back(*move)):
        to_gx, to_gy, shard = peer(move_of(group, member))
        there, place = back(group, member)
        pltpu.make_async_remote_copy(
            src_ref=want_ref.at[shard], dst_ref=asked.at[there * MEMBERS + place],
            send_sem=ask_send, recv_sem=ask_recv.at[there],
            device_id=(to_gx, to_gy), device_id_type=MESH,
        ).start()
    home = GROUPS.index((0, 0))
    asked[pl.ds(home * MEMBERS, 1)] = want_ref[pl.ds(me, 1)]
    for chunk in range(early, chunks):
        load(chunk)

    def number_copy(number):
        members = pl.ds(number * MEMBERS, MEMBERS)
        return pltpu.make_async_copy(asked.at[members], numbers.at[members], number_sems.at[number])

    def hear(number):
        heard = pl.ds(number * MEMBERS, MEMBERS)
        if number == home:
            heard = pl.ds(number * MEMBERS + 1, MEMBERS - 1)
        pltpu.make_async_copy(asked.at[heard], asked.at[heard], ask_recv.at[number]).wait()
        number_copy(number).start()

    def collect(place, shard):
        for slot in range(capacity):
            block[pl.ds(slot, 1)] = table[pl.ds(numbers[place, 0, slot], 1)]
        sending[shard] = block[...].astype(jnp.bfloat16)

    def receiver(group, member):
        a = member % 4
        to_gx = ((x + a) % 4) * 8 + ((y + a + group[0]) % 4) * 2 + (core + member // 4) % 2
        to_gy = (gy + a + group[1]) % 4
        return to_gx, to_gy, to_gx * 4 + to_gy

    def send(group, member):
        to_gx, to_gy, shard = receiver(group, member)
        pltpu.make_async_remote_copy(
            src_ref=sending.at[shard], dst_ref=out_ref.at[me], send_sem=row_send, recv_sem=row_recv,
            device_id=(to_gx, to_gy), device_id_type=MESH,
        ).start()

    hear(0)
    for number, group in enumerate(GROUPS):
        if number + 1 < len(GROUPS):
            hear(number + 1)
        number_copy(number).wait()
        if number:
            send(GROUPS[number - 1], MEMBERS - 1)
        first = 1 if number == home else 0

        def give(member, carry):
            collect(number * MEMBERS + member, receiver(group, member)[2])
            pl.when(member > first)(lambda: send(group, member - 1))
            return carry

        lax.fori_loop(first, MEMBERS, give, 0)
    collect(home * MEMBERS, me)
    send(GROUPS[-1], MEMBERS - 1)
    others = pl.ds(0, shards - 1)
    pltpu.make_async_copy(asked.at[others], asked.at[others], ask_send).wait()
    own = pltpu.make_async_copy(sending.at[me], out_ref.at[me], own_sem)
    own.start()
    own.wait()
    pltpu.make_async_copy(sending.at[others], sending.at[others], row_recv).wait()
    pltpu.make_async_copy(sending.at[others], sending.at[others], row_send).wait()


def exchange(want, item_table, capacity):
    shards, _, lanes = want.shape
    rows, width = item_table.shape
    chunks, ring, early = 12, 4, 6
    whole, anywhere = pl.BlockSpec(memory_space=pltpu.VMEM), pl.BlockSpec(memory_space=pl.ANY)
    return pl.pallas_call(
        functools.partial(
            exchange_kernel, shards=shards, chunks=chunks, early=early, capacity=capacity
        ),
        in_specs=[whole, anywhere],
        out_specs=anywhere,
        out_shape=jax.ShapeDtypeStruct((shards, capacity, width), jnp.bfloat16),
        scratch_shapes=[
            pltpu.VMEM((rows // chunks * ring, width), jnp.bfloat16),
            pltpu.VMEM((rows, width), jnp.float32),
            pltpu.VMEM((capacity, width), jnp.float32),
            pltpu.VMEM((shards, capacity, width), jnp.bfloat16),
            pltpu.VMEM((shards, 1, lanes), jnp.int32),
            pltpu.SMEM((shards, 1, lanes), jnp.int32),
            pltpu.SemaphoreType.DMA((ring,)),
            pltpu.SemaphoreType.DMA,
            pltpu.SemaphoreType.DMA((len(GROUPS),)),
            pltpu.SemaphoreType.DMA,
            pltpu.SemaphoreType.DMA,
            pltpu.SemaphoreType.DMA((len(GROUPS),)),
            pltpu.SemaphoreType.DMA,
        ],
        compiler_params=pltpu.CompilerParams(
            collective_id=0, has_side_effects=True, vmem_limit_bytes=52 * 1024 * 1024
        ),
        name="exchange",
    )(want, item_table)


def per_device(
    candidate_owner,
    candidate_row,
    item_table,
    w_in,
    w_qkv,
    w_out,
    w_up,
    w_down,
    norm_gains,
    final_gain,
    w_score,
):
    slates, length, unused = candidate_owner.shape
    width = item_table.shape[1]
    shards = lax.axis_size(("gx", "gy"))
    capacity = max(2, 2 * slates * length // shards)
    want, place = number_candidates(
        candidate_owner.reshape(slates, 1, length), candidate_row, shards, capacity
    )
    rows = exchange(want, item_table, capacity)
    rows = rows.reshape(shards * capacity, width)
    return score_slates(
        rows, place, w_in, w_qkv, w_out, w_up, w_down, norm_gains, final_gain, w_score
    )


def solution(mesh):
    return jax.shard_map(
        per_device,
        mesh=mesh,
        in_specs=(
            P(("gx", "gy"), None, None),
            P(("gx", "gy"), None),
            P(("gx", "gy"), None),
            P(),
            P(),
            P(),
            P(),
            P(),
            P(),
            P(),
            P(),
        ),
        out_specs=P(("gx", "gy"), None),
        check_vma=False,
    )
```
